32 devices in a mesh: gx: 2 (over y), gy: 4 (over z), gz: 4 (over x, core).
Axes of the slice: x: 2, y: 2, z: 4, core: 2. Of those that a mesh axis runs over, the one named last changes fastest.
Arguments:
- right_side: float32 [32, 64, 512], P('gx', 'gy', 'gz'), may hold values from -6 to 6
- coefficient: float32 [32, 64, 512], P('gx', 'gy', 'gz'), may hold values from 0.5 to 4
- start_vector: float32 [32, 64, 512], P('gx', 'gy', 'gz'), may hold values from -12 to 12
- plane_counts: int32 [4], replicated, may hold values from 32 to 128, as said below
Outputs:
- solution_field: float32 [32, 64, 512], P('gx', 'gy', 'gz')
- residual: float32 [32, 64, 512], P('gx', 'gy', 'gz')
The draws below stay inside these ranges and needn't reach their ends.
Inputs may be any that keep to these rules, and one draw needn't show every extreme that they name: plane_counts sum to 320, and the largest is exactly 128.
All inputs are finite; a program needn't handle non-finite values.
Results may differ from the reference program's by a relative error of at most 0.0003.
Values sent between devices are 32-bit elements; how exact they have to be, the bound alone decides.
A program may use at most 64 MiB of HBM per device.

```python
import math
import jax
import jax.numpy as jnp
from jax import lax

CAP = 128
POWER = 3
DEGREE = 4
PLANES = 80
NX = 32
NY = 64
NZ = 320
N_GZ = 4


def draw_start_vector(key, part):
    ramp = 1.0 + 2.0 * jnp.arange(NX, dtype=jnp.float32) / max(NX - 1, 1)
    layout = (NX, NY, N_GZ * CAP)
    base = jnp.clip(jax.random.normal(key, layout, jnp.float32), -4.0, 4.0)
    return base * ramp[:, None, None]


def draw_plane_counts(key, part):
    halves = N_GZ // 2
    key_order, key_spread, key_pick = jax.random.split(jax.random.fold_in(key, 7), 3)
    order = jax.random.permutation(key_order, N_GZ)
    spread = jax.random.randint(key_spread, (halves,), 0, CAP - PLANES + 1)
    chosen = jax.random.randint(key_pick, (), 0, halves)
    spread = jnp.where(jnp.arange(halves) == chosen, CAP - PLANES, spread)
    values = jnp.concatenate([PLANES + spread, PLANES - spread]).astype(jnp.int32)
    return jnp.zeros((N_GZ,), jnp.int32).at[order].set(values)


def shard_levels(own_key, extent, pieces, smallest, high):
    def one(dim, parts):
        steps = jax.random.uniform(jax.random.fold_in(jax.random.fold_in(own_key, 6), dim), (parts,), jnp.float32, smallest / len(pieces), high / len(pieces))
        return jnp.repeat(jnp.exp(steps), extent[dim] // parts).reshape((-1,) + (1,) * (len(extent) - dim - 1))

    level = one(*pieces[0])
    for cut in pieces[1:]:
        level = level * one(*cut)
    return level


def bell_draw(key, extent, scale, limit, shards=(), held_as=jnp.bfloat16):
    gain = shard_levels(key, extent, shards, -0.22, 0.18) if shards else 1.0
    entries = jax.random.normal(key, extent, jnp.float32) * scale * gain
    return jnp.minimum(jnp.maximum(entries, -limit), limit).astype(held_as)


def setup_inputs(seed: int = 0) -> dict:
    key_list = jax.random.split(jax.random.key(seed), 5)
    return {
        "right_side": bell_draw(key_list[0], (NX, NY, N_GZ * CAP), 1.0, 6.0, ((0, 2), (1, 4), (2, 4)), jnp.float32),
        "coefficient": jnp.clip(jnp.exp(math.log(4.0) - 2.0794415 * jax.random.uniform(key_list[1], (NX, NY, N_GZ * CAP), jnp.float32) ** shard_levels(key_list[1], (NX, NY, N_GZ * CAP), ((0, 2), (1, 4), (2, 4)), -0.2, 0.2)), 0.5, 4.0),
        "start_vector": draw_start_vector(jax.random.fold_in(key_list[4], 71), 0),
        "plane_counts": draw_plane_counts(jax.random.fold_in(key_list[4], 71), 0),
    }


def neighbours(field):
    return [field[2:, 1:-1, 1:-1], field[:-2, 1:-1, 1:-1], field[1:-1, 2:, 1:-1], field[1:-1, :-2, 1:-1], field[1:-1, 1:-1, 2:], field[1:-1, 1:-1, :-2]]

def apply_stencil(field, coefs):
    middle = field[1:-1, 1:-1, 1:-1]
    centre_coef = coefs[1:-1, 1:-1, 1:-1]
    accumulated = jnp.zeros_like(middle)
    for beside, other in zip(neighbours(field), neighbours(coefs)):
        other = jnp.where(other > 0, other, centre_coef)
        accumulated = accumulated + 0.5 * (centre_coef + other) * (middle - beside)
    return accumulated

def slot_maps(plane_counts):
    offsets = (jnp.cumsum(plane_counts) - plane_counts).astype(jnp.int32)
    cells = jnp.arange(NZ, dtype=jnp.int32)
    owner = lax.optimization_barrier(jnp.sum((cells[:, None] >= offsets[None, 1:]).astype(jnp.int32), axis=1)).astype(jnp.int32)
    source = (owner * CAP + cells - offsets[owner]).astype(jnp.int32)
    slots = jnp.arange(N_GZ * CAP, dtype=jnp.int32)
    holder = (slots // CAP).astype(jnp.int32)
    within = (slots % CAP).astype(jnp.int32)
    alive = within < plane_counts[holder]
    target = jnp.minimum(offsets[holder] + within, NZ - 1).astype(jnp.int32)
    return (source, alive, target)

def reference(right_side, coefficient, start_vector, plane_counts):
    source, alive, target = slot_maps(plane_counts)
    rhs = jnp.take(right_side, source, axis=2)
    coefs = jnp.take(coefficient, source, axis=2)
    start = jnp.take(start_vector, source, axis=2)
    padded_coefs = jnp.pad(coefs, 1)

    def operate(field):
        return apply_stencil(jnp.pad(field, 1), padded_coefs)
    vector = start / jnp.sqrt(jnp.sum(start * start))
    largest = jnp.float32(1.0)
    for sweep in range(POWER):
        image = operate(vector)
        largest = jnp.sqrt(jnp.sum(image * image))
        vector = image / largest
    center = 0.6 * largest
    half_width = 0.5 * largest
    sharpness = 1.2
    ratio = 1.0 / sharpness
    solution = jnp.zeros_like(rhs)
    residue = rhs
    direction = rhs / center
    for section in range(DEGREE):
        solution = solution + direction
        residue = residue - operate(direction)
        if section < DEGREE - 1:
            fresh = 1.0 / (2.0 * sharpness - ratio)
            direction = fresh * ratio * direction + 2.0 * fresh / half_width * residue
            ratio = fresh

    def back(field):
        return jnp.where(alive[None, None, :], jnp.take(field, target, axis=2), jnp.float32(0.0))
    return (back(solution), back(residue))
```

```python
import functools

import numpy as np
import jax
import jax.numpy as jnp
from jax import lax
from jax.experimental import pallas as pl
from jax.experimental.pallas import tpu as pltpu
from jax.sharding import PartitionSpec as P

POWER = 3
DEGREE = 4
AXES = ("gx", "gy", "gz")
SUM_ORDER = ("gz", "gx", "gy")
MESH = pl.DeviceIdType.MESH


def chebyshev_polynomials():
    basis = np.zeros(DEGREE + 2)
    basis[0] = 1.0
    times = lambda poly: np.concatenate([[0.0], poly[:-1]])
    sharpness = 1.2
    ratio = 1.0 / sharpness
    answer = np.zeros_like(basis)
    residue = basis.copy()
    direction = basis / 0.6
    for section in range(DEGREE):
        answer = answer + direction
        residue = residue - times(direction)
        if section < DEGREE - 1:
            fresh = 1.0 / (2.0 * sharpness - ratio)
            direction = fresh * ratio * direction + 2.0 * fresh / 0.5 * residue
            ratio = fresh
    return [float(v) for v in answer[:DEGREE]], [float(v) for v in residue[: DEGREE + 1]]


def kernel(
    sizes, counts_ref, rhs_ref, coef_ref, start_ref, sol_ref, res_ref,
    pow_ref, kry_ref, wx_ref, wym_ref, wyp_ref, wzm_ref, wzp_ref, diag_ref,
    sx, sy, sz, rx, ry, rz, sums_gz, sums_gx, sums_gy, send_sem, recv_sem, sum_send, sum_recv,
):
    X, Y, S = rhs_ref.shape
    me = {a: lax.axis_index(a) for a in AXES}
    has = {}
    for a in AXES:
        has[a] = (me[a] > 0, me[a] < sizes[a] - 1)

    barrier = pltpu.get_barrier_semaphore()
    for a in AXES:
        for step in range(1, sizes[a]):
            pl.semaphore_signal(
                barrier, inc=1, device_id={a: lax.rem(me[a] + step, sizes[a])}, device_id_type=MESH
            )

    lane = lax.broadcasted_iota(jnp.int32, (Y, S), 1)
    row = lax.broadcasted_iota(jnp.int32, (Y, S), 0)
    planes = counts_ref[me["gz"]]
    alive = lane < planes
    is_first = lane == 0
    is_last = lane == planes - 1
    top = row == 0
    bottom = row == Y - 1

    def descriptor(msg, fields, axis, side):
        send, recv, which = {"gx": (sx, rx, 0), "gy": (sy, ry, 1), "gz": (sz, rz, 2)}[axis]
        if axis == "gz":
            src, dst = send.at[msg, side], recv.at[msg, 1 - side]
        else:
            src = send.at[msg, side, pl.ds(0, fields)]
            dst = recv.at[msg, 1 - side, pl.ds(0, fields)]
        return pltpu.make_async_remote_copy(
            src_ref=src,
            dst_ref=dst,
            send_sem=send_sem.at[msg, which, side],
            recv_sem=recv_sem.at[msg, which, 1 - side],
            device_id={axis: me[axis] + (1 if side else -1)},
            device_id_type=MESH,
        )

    class Packer:
        def __init__(self, msg):
            self.msg = msg
            self.low = jnp.zeros((Y, S), jnp.float32)
            self.high = jnp.zeros((Y, S), jnp.float32)

        def put(self, f, x, value):
            m = self.msg
            if x == 0:
                sx[m, 0, f] = value
            if x == X - 1:
                sx[m, 1, f] = value
            sy[m, 0, f, x : x + 1, :] = value[0:1, :]
            sy[m, 1, f, x : x + 1, :] = value[Y - 1 : Y, :]
            here = lane == f * X + x
            self.low = jnp.where(here, value[:, 0:1], self.low)
            tail = jnp.sum(jnp.where(is_last, value, 0.0), axis=1, keepdims=True)
            self.high = jnp.where(here, tail, self.high)

        def finish(self):
            sz[self.msg, 0] = self.low
            sz[self.msg, 1] = self.high

    def launch(msg, fields):
        for axis in AXES:
            for side in (0, 1):
                @pl.when(has[axis][side])
                def _(axis=axis, side=side):
                    descriptor(msg, fields, axis, side).start()

    def receive(msg, fields):
        for axis in AXES:
            for side in (0, 1):
                @pl.when(has[axis][1 - side])
                def _(axis=axis, side=side):
                    descriptor(msg, fields, axis, side).wait_recv()

    def drain(msg, fields):
        for axis in AXES:
            for side in (0, 1):
                @pl.when(has[axis][side])
                def _(axis=axis, side=side):
                    descriptor(msg, fields, axis, side).wait_send()

    def blank():
        for axis, recv in (("gx", rx), ("gy", ry), ("gz", rz)):
            for side in (0, 1):
                @pl.when(jnp.logical_not(has[axis][side]))
                def _(recv=recv, side=side):
                    for msg in range(recv.shape[0]):
                        recv[msg, side] = jnp.zeros(recv.shape[2:], jnp.float32)

    def around(load, msg, f, x, zlow, zhigh):
        centre = load(x)
        below = rx[msg, 0, f] if x == 0 else load(x - 1)
        above = rx[msg, 1, f] if x == X - 1 else load(x + 1)
        ym = jnp.where(top, ry[msg, 0, f, x : x + 1, :], pltpu.roll(centre, 1, 0))
        yp = jnp.where(bottom, ry[msg, 1, f, x : x + 1, :], pltpu.roll(centre, Y - 1, 0))
        at = f * X + x
        zm = jnp.where(is_first, zlow[:, at : at + 1], pltpu.roll(centre, 1, 1))
        zp = jnp.where(is_last, zhigh[:, at : at + 1], pltpu.roll(centre, S - 1, 1))
        return centre, below, above, ym, yp, zm, zp

    def face(centre, other):
        other = jnp.where(other > 0, other, centre)
        return jnp.where(alive, 0.5 * (centre + other), 0.0)

    def weights(msg):
        zlow, zhigh = rz[msg, 0], rz[msg, 1]
        under = None
        for x in range(X):
            c, below, above, ym, yp, zm, zp = around(lambda i: coef_ref[i], msg, 0, x, zlow, zhigh)
            if x == 0:
                under = face(c, below)
                wx_ref[0] = under
            over = face(c, above)
            parts = [face(c, o) for o in (ym, yp, zm, zp)]
            wx_ref[x + 1] = over
            wym_ref[x], wyp_ref[x], wzm_ref[x], wzp_ref[x] = parts
            diag_ref[x] = (under + over) + (parts[0] + parts[1]) + (parts[2] + parts[3])
            under = over

    def operate(load, msg, f, emit):
        zlow, zhigh = rz[msg, 0], rz[msg, 1]
        for x in range(X):
            c, below, above, ym, yp, zm, zp = around(load, msg, f, x, zlow, zhigh)
            near = wx_ref[x] * below + wx_ref[x + 1] * above
            near = near + (wym_ref[x] * ym + wyp_ref[x] * yp)
            near = near + (wzm_ref[x] * zm + wzp_ref[x] * zp)
            emit(x, diag_ref[x] * c - near)

    def step(load, msg, f, store, out_msg, total=None):
        pack = Packer(out_msg) if out_msg is not None else None
        box = [total]

        def emit(x, value):
            if store is not None:
                store[x] = value
            if pack is not None:
                pack.put(0, x, value)
            if total is not None:
                box[0] = box[0] + value * value

        operate(load, msg, f, emit)
        if pack is not None:
            pack.finish()
            launch(out_msg, 1)
        return box[0]

    pack = Packer(0)
    for x in range(X):
        pack.put(0, x, coef_ref[x])
        pack.put(1, x, start_ref[x])
    pack.finish()
    pack = Packer(1)
    for x in range(X):
        pack.put(0, x, rhs_ref[x])
    pack.finish()
    blank()
    pl.semaphore_wait(barrier, sum(sizes[a] - 1 for a in AXES))
    launch(0, 2)
    launch(1, 1)

    zero = jnp.zeros((Y, S), jnp.float32)
    receive(0, 2)
    weights(0)
    step(lambda x: start_ref[x], 0, 1, pow_ref.at[0], 2)
    receive(1, 1)
    step(lambda x: rhs_ref[x], 1, 0, kry_ref.at[0], 4)
    receive(2, 1)
    lower = step(lambda x: pow_ref[0, x], 2, 0, pow_ref.at[1], 3, zero)
    receive(4, 1)
    step(lambda x: kry_ref[0, x], 4, 0, kry_ref.at[1], 5)
    receive(3, 1)
    upper = step(lambda x: pow_ref[1, x], 3, 0, None, None, zero)

    sums = {"gz": sums_gz, "gx": sums_gx, "gy": sums_gy}
    pick = lax.broadcasted_iota(jnp.int32, (8, S), 0) < 4
    mine = jnp.where(pick, jnp.sum(upper, keepdims=True), jnp.sum(lower, keepdims=True))

    def sum_copy(k, axis, peer):
        buf = sums[axis]
        return pltpu.make_async_remote_copy(
            src_ref=buf.at[me[axis]],
            dst_ref=buf.at[me[axis]],
            send_sem=sum_send.at[k, peer],
            recv_sem=sum_recv.at[k, me[axis]],
            device_id={axis: peer},
            device_id_type=MESH,
        )

    def sum_arrival(k, axis, peer):
        buf = sums[axis]
        return pltpu.make_async_remote_copy(
            src_ref=buf.at[peer],
            dst_ref=buf.at[peer],
            send_sem=sum_send.at[k, peer],
            recv_sem=sum_recv.at[k, peer],
            device_id={axis: peer},
            device_id_type=MESH,
        )

    def sums_out(k, value):
        axis = SUM_ORDER[k]
        sums[axis][me[axis]] = value
        for hop in range(1, sizes[axis]):
            sum_copy(k, axis, lax.rem(me[axis] + hop, sizes[axis])).start()

    def sums_in(k):
        axis = SUM_ORDER[k]
        for hop in range(1, sizes[axis]):
            sum_arrival(k, axis, lax.rem(me[axis] + hop, sizes[axis])).wait_recv()
        value = sums[axis][0]
        for i in range(1, sizes[axis]):
            value = value + sums[axis][i]
        return value

    sums_out(0, mine)
    receive(5, 1)
    step(lambda x: kry_ref[1, x], 5, 0, kry_ref.at[2], 6)
    sums_out(1, sums_in(0))
    receive(6, 1)
    step(lambda x: kry_ref[2, x], 6, 0, kry_ref.at[3], None)
    sums_out(2, sums_in(1))
    total = sums_in(2)
    inverse = jnp.sqrt(total[4:5, :] / total[0:1, :])
    answer, residue = chebyshev_polynomials()
    power = [jnp.ones_like(inverse)]
    for _ in range(DEGREE):
        power.append(power[-1] * inverse)
    for x in range(X):
        krylov = [jnp.where(alive, rhs_ref[x], 0.0)] + [kry_ref[i, x] for i in range(DEGREE)]
        sol = krylov[0] * (answer[0] * power[1])
        res = krylov[0] * residue[0]
        for i in range(1, DEGREE):
            sol = sol + krylov[i] * (answer[i] * power[i + 1])
        for i in range(1, DEGREE + 1):
            res = res + krylov[i] * (residue[i] * power[i])
        sol_ref[x] = sol
        res_ref[x] = res

    drain(0, 2)
    for msg in range(1, 7):
        drain(msg, 1)
    for k, axis in enumerate(SUM_ORDER):
        for hop in range(1, sizes[axis]):
            sum_copy(k, axis, lax.rem(me[axis] + hop, sizes[axis])).wait_send()


def on_device(sizes, right_side, coefficient, start_vector, plane_counts):
    X, Y, S = right_side.shape
    f32 = jnp.float32
    most = max(sizes.values())
    vmem = pl.BlockSpec(memory_space=pltpu.VMEM)
    return pl.pallas_call(
        functools.partial(kernel, sizes),
        out_shape=(jax.ShapeDtypeStruct((X, Y, S), f32),) * 2,
        in_specs=[pl.BlockSpec(memory_space=pltpu.SMEM), vmem, vmem, vmem],
        out_specs=(vmem, vmem),
        scratch_shapes=[
            pltpu.VMEM((POWER - 1, X, Y, S), f32),
            pltpu.VMEM((DEGREE, X, Y, S), f32),
            pltpu.VMEM((X + 1, Y, S), f32),
            *[pltpu.VMEM((X, Y, S), f32)] * 5,
            pltpu.VMEM((7, 2, 2, Y, S), f32),
            pltpu.VMEM((7, 2, 2, X, S), f32),
            pltpu.VMEM((7, 2, Y, S), f32),
            pltpu.VMEM((7, 2, 2, Y, S), f32),
            pltpu.VMEM((7, 2, 2, X, S), f32),
            pltpu.VMEM((7, 2, Y, S), f32),
            pltpu.VMEM((sizes["gz"], 8, S), f32),
            pltpu.VMEM((sizes["gx"], 8, S), f32),
            pltpu.VMEM((sizes["gy"], 8, S), f32),
            pltpu.SemaphoreType.DMA((7, 3, 2)),
            pltpu.SemaphoreType.DMA((7, 3, 2)),
            pltpu.SemaphoreType.DMA((3, most)),
            pltpu.SemaphoreType.DMA((3, most)),
        ],
        compiler_params=pltpu.CompilerParams(collective_id=0, has_side_effects=True),
    )(plane_counts, right_side, coefficient, start_vector)


def solution(mesh):
    sizes = {a: mesh.shape[a] for a in AXES}
    spec = P("gx", "gy", "gz")
    return jax.shard_map(
        functools.partial(on_device, sizes),
        mesh=mesh,
        in_specs=(spec, spec, spec, P()),
        out_specs=(spec, spec),
        check_vma=False,
    )
```

```python
import functools

import numpy as np
import jax
import jax.numpy as jnp
from jax import lax
from jax.experimental import pallas as pl
from jax.experimental.pallas import tpu as pltpu
from jax.sharding import PartitionSpec as P

POWER = 3
DEGREE = 4
AXES = ("gx", "gy", "gz")
DIRECT_LIMIT = 64
START, RIGHT, V1, V2, K1, K2, K3 = range(7)
ENTRIES = {START: (0, 2, 0), RIGHT: (2, 1, 2), V1: (3, 1, 1), V2: (4, 1, 0), K1: (5, 1, 3), K2: (6, 1, 2), K3: (7, 1, 3)}
MESH = pl.DeviceIdType.MESH


def chebyshev_polynomials():
    basis = np.zeros(DEGREE + 2)
    basis[0] = 1.0
    times = lambda poly: np.concatenate([[0.0], poly[:-1]])
    sharpness = 1.2
    ratio = 1.0 / sharpness
    answer = np.zeros_like(basis)
    residue = basis.copy()
    direction = basis / 0.6
    for section in range(DEGREE):
        answer = answer + direction
        residue = residue - times(direction)
        if section < DEGREE - 1:
            fresh = 1.0 / (2.0 * sharpness - ratio)
            direction = fresh * ratio * direction + 2.0 * fresh / 0.5 * residue
            ratio = fresh
    return [float(v) for v in answer[:DEGREE]], [float(v) for v in residue[: DEGREE + 1]]


def plan(sizes):
    if sizes["gx"] * sizes["gy"] * sizes["gz"] <= DIRECT_LIMIT:
        return (("gx", "gy", "gz"),), sum(sizes.values()) - len(sizes) - 1
    return (("gz",), ("gx",), ("gy",)), 0


def offsets(sizes, axes):
    grid = list(np.ndindex(*[sizes[a] for a in axes]))
    return [dict(zip(axes, map(int, o))) for o in grid if any(o)]


def kernel(
    sizes, counts_ref, rhs_ref, coef_ref, start_ref, kry_out, total_ref,
    pow_ref, kry_ref, wx_ref, wym_ref, wyp_ref, wzm_ref, wzp_ref, diag_ref,
    sx, sy, sz, rx, ry, rz, own_ref, sums_ref, send_sem, recv_sem, sum_send, sum_recv, out_sem, flood_sem,
):
    X, Y, S = rhs_ref.shape
    me = {a: lax.axis_index(a) for a in AXES}
    stages, floods = plan(sizes)
    has = {}
    for a in AXES:
        has[a] = (me[a] > 0, me[a] < sizes[a] - 1)
    neighbours = sum(h.astype(jnp.int32) for a in AXES for h in has[a])

    def greet(sem):
        for a in AXES:
            for side in (0, 1):
                @pl.when(has[a][side])
                def _(a=a, side=side):
                    pl.semaphore_signal(
                        sem, inc=1, device_id={a: me[a] + (1 if side else -1)}, device_id_type=MESH
                    )

    flooded = [0]

    def flood(rounds):
        for _ in range(rounds):
            if flooded[0] < floods:
                greet(flood_sem.at[flooded[0]])
                pl.semaphore_wait(flood_sem.at[flooded[0]], neighbours)
                flooded[0] += 1

    barrier = pltpu.get_barrier_semaphore()
    if floods:
        greet(barrier)
        arrivals = neighbours
    else:
        for a in AXES:
            for step in range(1, sizes[a]):
                pl.semaphore_signal(
                    barrier, inc=1, device_id={a: lax.rem(me[a] + step, sizes[a])}, device_id_type=MESH
                )
        arrivals = sum(sizes[a] - 1 for a in AXES)

    lane = lax.broadcasted_iota(jnp.int32, (Y, S), 1)
    row = lax.broadcasted_iota(jnp.int32, (Y, S), 0)
    planes = counts_ref[me["gz"]]
    alive = lane < planes
    is_first = lane == 0
    is_last = lane == planes - 1
    top = row == 0
    bottom = row == Y - 1

    def descriptor(msg, axis, side):
        send, recv, which = {"gx": (sx, rx, 0), "gy": (sy, ry, 1), "gz": (sz, rz, 2)}[axis]
        entry, fields, arrival = ENTRIES[msg]
        at = msg if axis == "gz" else pl.ds(entry, fields)
        return pltpu.make_async_remote_copy(
            src_ref=send.at[side, at],
            dst_ref=recv.at[1 - side, at],
            send_sem=send_sem.at[which, side],
            recv_sem=recv_sem.at[arrival, which, 1 - side],
            device_id={axis: me[axis] + (1 if side else -1)},
            device_id_type=MESH,
        )

    class Packer:
        def __init__(self, msg):
            self.msg = msg
            self.low = jnp.zeros((Y, S), jnp.float32)
            self.high = jnp.zeros((Y, S), jnp.float32)

        def put(self, f, x, value):
            e = ENTRIES[self.msg][0] + f
            if x == 0:
                sx[0, e] = value
            if x == X - 1:
                sx[1, e] = value
            sy[0, e, x : x + 1, :] = value[0:1, :]
            sy[1, e, x : x + 1, :] = value[Y - 1 : Y, :]
            here = lane == f * X + x
            self.low = jnp.where(here, value[:, 0:1], self.low)
            tail = jnp.sum(jnp.where(is_last, value, 0.0), axis=1, keepdims=True)
            self.high = jnp.where(here, tail, self.high)

        def finish(self):
            sz[0, self.msg] = self.low
            sz[1, self.msg] = self.high

    def launch(msg):
        for axis in AXES:
            for side in (0, 1):
                @pl.when(has[axis][side])
                def _(axis=axis, side=side):
                    descriptor(msg, axis, side).start()

    def receive(msg):
        for axis in AXES:
            for side in (0, 1):
                @pl.when(has[axis][1 - side])
                def _(axis=axis, side=side):
                    descriptor(msg, axis, side).wait_recv()

    def drain():
        for which, (axis, send, recv) in enumerate((("gx", sx, rx), ("gy", sy, ry), ("gz", sz, rz))):
            for side in (0, 1):
                @pl.when(has[axis][side])
                def _(axis=axis, side=side, which=which, send=send, recv=recv):
                    pltpu.make_async_remote_copy(
                        src_ref=send.at[side],
                        dst_ref=recv.at[1 - side],
                        send_sem=send_sem.at[which, side],
                        recv_sem=recv_sem.at[0, which, 1 - side],
                        device_id={axis: me[axis] + (1 if side else -1)},
                        device_id_type=MESH,
                    ).wait_send()

    def blank():
        for axis, recv in (("gx", rx), ("gy", ry), ("gz", rz)):
            for side in (0, 1):
                @pl.when(jnp.logical_not(has[axis][side]))
                def _(recv=recv, side=side):
                    recv[side] = jnp.zeros(recv.shape[1:], jnp.float32)

    def around(load, msg, f, x, zlow, zhigh):
        centre = load(x)
        below = rx[0, ENTRIES[msg][0] + f] if x == 0 else load(x - 1)
        above = rx[1, ENTRIES[msg][0] + f] if x == X - 1 else load(x + 1)
        ym = jnp.where(top, ry[0, ENTRIES[msg][0] + f, x : x + 1, :], pltpu.roll(centre, 1, 0))
        yp = jnp.where(bottom, ry[1, ENTRIES[msg][0] + f, x : x + 1, :], pltpu.roll(centre, Y - 1, 0))
        at = f * X + x
        zm = jnp.where(is_first, zlow[:, at : at + 1], pltpu.roll(centre, 1, 1))
        zp = jnp.where(is_last, zhigh[:, at : at + 1], pltpu.roll(centre, S - 1, 1))
        return centre, below, above, ym, yp, zm, zp

    def face(centre, other):
        other = jnp.where(other > 0, other, centre)
        return jnp.where(alive, 0.5 * (centre + other), 0.0)

    def weights(msg):
        zlow, zhigh = rz[0, msg], rz[1, msg]
        under = None
        for x in range(X):
            c, below, above, ym, yp, zm, zp = around(lambda i: coef_ref[i], msg, 0, x, zlow, zhigh)
            if x == 0:
                under = face(c, below)
                wx_ref[0] = under
            over = face(c, above)
            parts = [face(c, o) for o in (ym, yp, zm, zp)]
            wx_ref[x + 1] = over
            wym_ref[x], wyp_ref[x], wzm_ref[x], wzp_ref[x] = parts
            diag_ref[x] = (under + over) + (parts[0] + parts[1]) + (parts[2] + parts[3])
            under = over

    def operate(load, msg, f, emit):
        zlow, zhigh = rz[0, msg], rz[1, msg]
        for x in range(X):
            c, below, above, ym, yp, zm, zp = around(load, msg, f, x, zlow, zhigh)
            near = wx_ref[x] * below + wx_ref[x + 1] * above
            near = near + (wym_ref[x] * ym + wyp_ref[x] * yp)
            near = near + (wzm_ref[x] * zm + wzp_ref[x] * zp)
            emit(x, diag_ref[x] * c - near)

    def step(load, msg, f, store, out_msg, total=None):
        pack = Packer(out_msg) if out_msg is not None else None
        box = [total]

        def emit(x, value):
            if store is not None:
                store[x] = value
            if pack is not None:
                pack.put(0, x, value)
            if total is not None:
                box[0] = box[0] + value * value

        operate(load, msg, f, emit)
        if pack is not None:
            pack.finish()
            launch(out_msg)
        return box[0]

    pack = Packer(START)
    for x in range(X):
        pack.put(0, x, coef_ref[x])
        pack.put(1, x, start_ref[x])
    pack.finish()
    pack = Packer(RIGHT)
    for x in range(X):
        pack.put(0, x, rhs_ref[x])
    pack.finish()
    blank()
    pl.semaphore_wait(barrier, arrivals)
    launch(START)
    launch(RIGHT)

    def out_copy(i):
        return pltpu.make_async_copy(kry_ref.at[i], kry_out.at[i], out_sem.at[i])

    def krylov(i):
        source, msg, out_msg = ((None, RIGHT, K1), (0, K1, K2), (1, K2, K3), (2, K3, None))[i]
        load = (lambda x: rhs_ref[x]) if source is None else (lambda x: kry_ref[source, x])
        receive(msg)
        step(load, msg, 0, kry_ref.at[i], out_msg)
        out_copy(i).start()

    zero = jnp.zeros((Y, S), jnp.float32)
    flood(2)
    receive(START)
    weights(START)
    step(lambda x: start_ref[x], START, 1, pow_ref.at[0], V1)
    krylov(0)
    flood(2)
    receive(V1)
    lower = step(lambda x: pow_ref[0, x], V1, 0, pow_ref.at[1], V2, zero)
    krylov(1)
    flood(floods)
    receive(V2)
    upper = step(lambda x: pow_ref[1, x], V2, 0, None, None, zero)

    pick = lax.broadcasted_iota(jnp.int32, (8, S), 1) < S // 2
    total = jnp.where(pick, jnp.sum(upper, keepdims=True), jnp.sum(lower, keepdims=True))

    def sum_copy(k, slot, offset):
        return pltpu.make_async_remote_copy(
            src_ref=own_ref.at[k, pl.ds(0, 1)],
            dst_ref=sums_ref.at[k, pl.ds(slot, 1)],
            send_sem=sum_send.at[k],
            recv_sem=sum_recv.at[k],
            device_id={a: lax.rem(me[a] + d, sizes[a]) for a, d in offset.items()},
            device_id_type=MESH,
        )

    def all_sums(k, count):
        whole = sums_ref.at[k, pl.ds(0, count)]
        return pltpu.make_async_remote_copy(
            src_ref=whole,
            dst_ref=whole,
            send_sem=sum_send.at[k],
            recv_sem=sum_recv.at[k],
            device_id={"gz": lax.rem(me["gz"] + 1, sizes["gz"])},
            device_id_type=MESH,
        )

    for k, axes in enumerate(stages):
        own_ref[k] = total
        others = offsets(sizes, axes)
        for slot, offset in enumerate(others):
            sum_copy(k, slot, offset).start()
        if k == 0:
            krylov(2)
        if k == len(stages) - 1:
            krylov(3)
        all_sums(k, len(others)).wait_recv()
        total = total + jnp.sum(sums_ref[k, 0 : len(others), :], axis=0, keepdims=True)
    total_ref[...] = total
    for i in range(DEGREE):
        out_copy(i).wait()
    drain()
    for k, axes in enumerate(stages):
        all_sums(k, len(offsets(sizes, axes))).wait_send()


def combine(counts_ref, total_ref, rhs_ref, kry_ref, sol_ref, res_ref):
    X, Y, S = rhs_ref.shape
    alive = lax.broadcasted_iota(jnp.int32, (Y, S), 1) < counts_ref[lax.axis_index("gz")]
    inverse = jnp.sqrt(total_ref[0:1, S - 1 : S] / total_ref[0:1, 0:1])
    power = [jnp.ones_like(inverse)]
    for _ in range(DEGREE):
        power.append(power[-1] * inverse)
    answer, residue = chebyshev_polynomials()
    scale_sol = [jnp.broadcast_to(answer[i] * power[i + 1], (Y, S)) for i in range(DEGREE)]
    scale_res = [jnp.broadcast_to(residue[i] * power[i], (Y, S)) for i in range(DEGREE + 1)]
    for x in range(X):
        terms = [jnp.where(alive, rhs_ref[x], 0.0)] + [kry_ref[i, x] for i in range(DEGREE)]
        sol_ref[x] = sum(terms[i] * scale_sol[i] for i in range(DEGREE))
        res_ref[x] = sum(terms[i] * scale_res[i] for i in range(DEGREE + 1))


def on_device(sizes, right_side, coefficient, start_vector, plane_counts):
    X, Y, S = right_side.shape
    f32 = jnp.float32
    stages, floods = plan(sizes)
    most = max(len(offsets(sizes, axes)) for axes in stages)
    vmem = pl.BlockSpec(memory_space=pltpu.VMEM)
    krylov, total = pl.pallas_call(
        functools.partial(kernel, sizes),
        out_shape=(jax.ShapeDtypeStruct((DEGREE, X, Y, S), f32), jax.ShapeDtypeStruct((8, S), f32)),
        in_specs=[pl.BlockSpec(memory_space=pltpu.SMEM), vmem, vmem, vmem],
        out_specs=(pl.BlockSpec(memory_space=pl.ANY), vmem),
        scratch_shapes=[
            pltpu.VMEM((POWER - 1, X, Y, S), f32),
            pltpu.VMEM((DEGREE, X, Y, S), f32),
            pltpu.VMEM((X + 1, Y, S), f32),
            *[pltpu.VMEM((X, Y, S), f32)] * 5,
            *[pltpu.VMEM((2, 8, Y, S), f32), pltpu.VMEM((2, 8, X, S), f32), pltpu.VMEM((2, 7, Y, S), f32)] * 2,
            pltpu.VMEM((len(stages), 8, S), f32),
            pltpu.VMEM((len(stages), -(-most // 8) * 8, S), f32),
            pltpu.SemaphoreType.DMA((3, 2)),
            pltpu.SemaphoreType.DMA((4, 3, 2)),
            pltpu.SemaphoreType.DMA((len(stages),)),
            pltpu.SemaphoreType.DMA((len(stages),)),
            pltpu.SemaphoreType.DMA((DEGREE,)),
            pltpu.SemaphoreType.REGULAR((max(floods, 1),)),
        ],
        compiler_params=pltpu.CompilerParams(collective_id=0, has_side_effects=True),
    )(plane_counts, right_side, coefficient, start_vector)
    return pl.pallas_call(
        combine,
        out_shape=(jax.ShapeDtypeStruct((X, Y, S), f32),) * 2,
        in_specs=[pl.BlockSpec(memory_space=pltpu.SMEM), vmem, vmem, vmem],
        out_specs=(vmem, vmem),
    )(plane_counts, total, right_side, krylov)


def solution(mesh):
    sizes = {a: mesh.shape[a] for a in AXES}
    spec = P("gx", "gy", "gz")
    return jax.shard_map(
        functools.partial(on_device, sizes),
        mesh=mesh,
        in_specs=(spec, spec, spec, P()),
        out_specs=(spec, spec),
        check_vma=False,
    )
```

```python
import functools

import numpy as np
import jax
import jax.numpy as jnp
from jax import lax
from jax.experimental import pallas as pl
from jax.experimental.pallas import tpu as pltpu
from jax.sharding import PartitionSpec as P

POWER = 3
DEGREE = 4
AXES = ("gx", "gy", "gz")
DIRECT_LIMIT = 64
START, RIGHT, V1, V2, K1, K2, K3 = range(7)
ENTRIES = {START: (0, 2, 0), RIGHT: (2, 1, 2), V1: (3, 1, 1), V2: (4, 1, 0), K1: (5, 1, 3), K2: (6, 1, 2), K3: (7, 1, 3)}
MESH = pl.DeviceIdType.MESH


def chebyshev_polynomials():
    basis = np.zeros(DEGREE + 2)
    basis[0] = 1.0
    times = lambda poly: np.concatenate([[0.0], poly[:-1]])
    sharpness = 1.2
    ratio = 1.0 / sharpness
    answer = np.zeros_like(basis)
    residue = basis.copy()
    direction = basis / 0.6
    for section in range(DEGREE):
        answer = answer + direction
        residue = residue - times(direction)
        if section < DEGREE - 1:
            fresh = 1.0 / (2.0 * sharpness - ratio)
            direction = fresh * ratio * direction + 2.0 * fresh / 0.5 * residue
            ratio = fresh
    return [float(v) for v in answer[:DEGREE]], [float(v) for v in residue[: DEGREE + 1]]


def plan(sizes):
    if sizes["gx"] * sizes["gy"] * sizes["gz"] <= DIRECT_LIMIT:
        return (("gx", "gy", "gz"),), max(sum(sizes.values()) - len(sizes) - 2, 1)
    return (("gz",), ("gx",), ("gy",)), 0


def offsets(sizes, axes):
    grid = list(np.ndindex(*[sizes[a] for a in axes]))
    return [dict(zip(axes, map(int, o))) for o in grid if any(o)]


def kernel(
    sizes, counts_ref, rhs_hbm, coef_hbm, start_hbm, kry_out, total_ref, rhs_ref, coef_ref, start_ref,
    pow_ref, kry_ref, wx_ref, wym_ref, wyp_ref, wzm_ref, wzp_ref, diag_ref,
    sx, sy, sz, rx, ry, rz, own_ref, sums_ref, send_sem, recv_sem, sum_send, sum_recv, out_sem, flood_sem, in_sem,
):
    X, Y, S = rhs_ref.shape
    me = {a: lax.axis_index(a) for a in AXES}
    stages, floods = plan(sizes)
    loads = [
        pltpu.make_async_copy(src, dst, in_sem.at[i])
        for i, (src, dst) in enumerate(((coef_hbm, coef_ref), (start_hbm, start_ref), (rhs_hbm, rhs_ref)))
    ]
    for load in loads:
        load.start()
    has = {}
    for a in AXES:
        has[a] = (me[a] > 0, me[a] < sizes[a] - 1)
    neighbours = sum(h.astype(jnp.int32) for a in AXES for h in has[a])

    def greet(sem):
        for a in AXES:
            for side in (0, 1):
                @pl.when(has[a][side])
                def _(a=a, side=side):
                    pl.semaphore_signal(
                        sem, inc=1, device_id={a: me[a] + (1 if side else -1)}, device_id_type=MESH
                    )

    flooded = [0]

    def flood(rounds):
        for _ in range(rounds):
            if flooded[0] < floods:
                greet(flood_sem.at[flooded[0]])
                pl.semaphore_wait(flood_sem.at[flooded[0]], neighbours)
                flooded[0] += 1

    barrier = pltpu.get_barrier_semaphore()
    if floods:
        greet(barrier)
        arrivals = neighbours
    else:
        for a in AXES:
            for step in range(1, sizes[a]):
                pl.semaphore_signal(
                    barrier, inc=1, device_id={a: lax.rem(me[a] + step, sizes[a])}, device_id_type=MESH
                )
        arrivals = sum(sizes[a] - 1 for a in AXES)

    lane = lax.broadcasted_iota(jnp.int32, (Y, S), 1)
    row = lax.broadcasted_iota(jnp.int32, (Y, S), 0)
    planes = counts_ref[me["gz"]]
    alive = lane < planes
    is_first = lane == 0
    is_last = lane == planes - 1
    top = row == 0
    bottom = row == Y - 1

    def descriptor(msg, axis, side):
        send, recv, which = {"gx": (sx, rx, 0), "gy": (sy, ry, 1), "gz": (sz, rz, 2)}[axis]
        entry, fields, arrival = ENTRIES[msg]
        at = msg if axis == "gz" else pl.ds(entry, fields)
        return pltpu.make_async_remote_copy(
            src_ref=send.at[side, at],
            dst_ref=recv.at[1 - side, at],
            send_sem=send_sem.at[which, side],
            recv_sem=recv_sem.at[arrival, which, 1 - side],
            device_id={axis: me[axis] + (1 if side else -1)},
            device_id_type=MESH,
        )

    class Packer:
        def __init__(self, msg):
            self.msg = msg
            self.low = jnp.zeros((Y, S), jnp.float32)
            self.high = jnp.zeros((Y, S), jnp.float32)

        def put(self, f, x, value):
            e = ENTRIES[self.msg][0] + f
            if x == 0:
                sx[0, e] = value
            if x == X - 1:
                sx[1, e] = value
            sy[0, e, x : x + 1, :] = value[0:1, :]
            sy[1, e, x : x + 1, :] = value[Y - 1 : Y, :]
            here = lane == f * X + x
            self.low = jnp.where(here, value[:, 0:1], self.low)
            tail = jnp.sum(jnp.where(is_last, value, 0.0), axis=1, keepdims=True)
            self.high = jnp.where(here, tail, self.high)

        def finish(self):
            sz[0, self.msg] = self.low
            sz[1, self.msg] = self.high

    def launch(msg):
        for axis in AXES:
            for side in (0, 1):
                @pl.when(has[axis][side])
                def _(axis=axis, side=side):
                    descriptor(msg, axis, side).start()

    def receive(msg):
        for axis in AXES:
            for side in (0, 1):
                @pl.when(has[axis][1 - side])
                def _(axis=axis, side=side):
                    descriptor(msg, axis, side).wait_recv()

    def drain():
        for which, (axis, send, recv) in enumerate((("gx", sx, rx), ("gy", sy, ry), ("gz", sz, rz))):
            for side in (0, 1):
                @pl.when(has[axis][side])
                def _(axis=axis, side=side, which=which, send=send, recv=recv):
                    pltpu.make_async_remote_copy(
                        src_ref=send.at[side],
                        dst_ref=recv.at[1 - side],
                        send_sem=send_sem.at[which, side],
                        recv_sem=recv_sem.at[0, which, 1 - side],
                        device_id={axis: me[axis] + (1 if side else -1)},
                        device_id_type=MESH,
                    ).wait_send()

    def blank():
        for axis, recv in (("gx", rx), ("gy", ry), ("gz", rz)):
            for side in (0, 1):
                @pl.when(jnp.logical_not(has[axis][side]))
                def _(recv=recv, side=side):
                    recv[side] = jnp.zeros(recv.shape[1:], jnp.float32)

    def around(load, msg, f, x, zlow, zhigh):
        centre = load(x)
        below = rx[0, ENTRIES[msg][0] + f] if x == 0 else load(x - 1)
        above = rx[1, ENTRIES[msg][0] + f] if x == X - 1 else load(x + 1)
        ym = jnp.where(top, ry[0, ENTRIES[msg][0] + f, x : x + 1, :], pltpu.roll(centre, 1, 0))
        yp = jnp.where(bottom, ry[1, ENTRIES[msg][0] + f, x : x + 1, :], pltpu.roll(centre, Y - 1, 0))
        at = f * X + x
        zm = jnp.where(is_first, zlow[:, at : at + 1], pltpu.roll(centre, 1, 1))
        zp = jnp.where(is_last, zhigh[:, at : at + 1], pltpu.roll(centre, S - 1, 1))
        return centre, below, above, ym, yp, zm, zp

    def face(centre, other):
        other = jnp.where(other > 0, other, centre)
        return jnp.where(alive, 0.5 * (centre + other), 0.0)

    def weights(msg):
        zlow, zhigh = rz[0, msg], rz[1, msg]
        under = None
        for x in range(X):
            c, below, above, ym, yp, zm, zp = around(lambda i: coef_ref[i], msg, 0, x, zlow, zhigh)
            if x == 0:
                under = face(c, below)
                wx_ref[0] = under
            over = face(c, above)
            parts = [face(c, o) for o in (ym, yp, zm, zp)]
            wx_ref[x + 1] = over
            wym_ref[x], wyp_ref[x], wzm_ref[x], wzp_ref[x] = parts
            diag_ref[x] = (under + over) + (parts[0] + parts[1]) + (parts[2] + parts[3])
            under = over

    def operate(load, msg, f, emit):
        zlow, zhigh = rz[0, msg], rz[1, msg]
        for x in range(X):
            c, below, above, ym, yp, zm, zp = around(load, msg, f, x, zlow, zhigh)
            near = wx_ref[x] * below + wx_ref[x + 1] * above
            near = near + (wym_ref[x] * ym + wyp_ref[x] * yp)
            near = near + (wzm_ref[x] * zm + wzp_ref[x] * zp)
            emit(x, diag_ref[x] * c - near)

    def step(load, msg, f, store, out_msg, total=None):
        pack = Packer(out_msg) if out_msg is not None else None
        box = [total]

        def emit(x, value):
            if store is not None:
                store[x] = value
            if pack is not None:
                pack.put(0, x, value)
            if total is not None:
                box[0] = box[0] + value * value

        operate(load, msg, f, emit)
        if pack is not None:
            pack.finish()
            launch(out_msg)
        return box[0]

    blank()
    loads[0].wait()
    loads[1].wait()
    pack = Packer(START)
    for x in range(X):
        pack.put(0, x, coef_ref[x])
        pack.put(1, x, start_ref[x])
    pack.finish()
    pl.semaphore_wait(barrier, arrivals)
    launch(START)
    loads[2].wait()
    pack = Packer(RIGHT)
    for x in range(X):
        pack.put(0, x, rhs_ref[x])
    pack.finish()
    launch(RIGHT)

    def out_copy(i):
        return pltpu.make_async_copy(kry_ref.at[i], kry_out.at[i], out_sem.at[i])

    def krylov(i):
        source, msg, out_msg = ((None, RIGHT, K1), (0, K1, K2), (1, K2, K3), (2, K3, None))[i]
        load = (lambda x: rhs_ref[x]) if source is None else (lambda x: kry_ref[source, x])
        receive(msg)
        step(load, msg, 0, kry_ref.at[i], out_msg)
        out_copy(i).start()

    zero = jnp.zeros((Y, S), jnp.float32)
    flood(3)
    receive(START)
    weights(START)
    step(lambda x: start_ref[x], START, 1, pow_ref.at[0], V1)
    krylov(0)
    receive(V1)
    lower = step(lambda x: pow_ref[0, x], V1, 0, pow_ref.at[1], V2, zero)
    krylov(1)
    flood(floods)
    receive(V2)
    upper = step(lambda x: pow_ref[1, x], V2, 0, None, None, zero)

    pick = lax.broadcasted_iota(jnp.int32, (8, S), 1) < S // 2
    total = jnp.where(pick, jnp.sum(upper, keepdims=True), jnp.sum(lower, keepdims=True))

    def sum_copy(k, slot, offset):
        return pltpu.make_async_remote_copy(
            src_ref=own_ref.at[k, pl.ds(0, 1)],
            dst_ref=sums_ref.at[k, pl.ds(slot, 1)],
            send_sem=sum_send.at[k],
            recv_sem=sum_recv.at[k],
            device_id={a: lax.rem(me[a] + d, sizes[a]) for a, d in offset.items()},
            device_id_type=MESH,
        )

    def all_sums(k, count):
        whole = sums_ref.at[k, pl.ds(0, count)]
        return pltpu.make_async_remote_copy(
            src_ref=whole,
            dst_ref=whole,
            send_sem=sum_send.at[k],
            recv_sem=sum_recv.at[k],
            device_id={"gz": lax.rem(me["gz"] + 1, sizes["gz"])},
            device_id_type=MESH,
        )

    for k, axes in enumerate(stages):
        own_ref[k] = total
        others = offsets(sizes, axes)
        for slot, offset in enumerate(others):
            sum_copy(k, slot, offset).start()
        if k == 0:
            krylov(2)
        if k == len(stages) - 1:
            krylov(3)
        all_sums(k, len(others)).wait_recv()
        total = total + jnp.sum(sums_ref[k, 0 : len(others), :], axis=0, keepdims=True)
    total_ref[...] = total
    for i in range(DEGREE):
        out_copy(i).wait()
    drain()
    for k, axes in enumerate(stages):
        all_sums(k, len(offsets(sizes, axes))).wait_send()


def combine(counts_ref, total_ref, rhs_ref, kry_ref, sol_ref, res_ref):
    X, Y, S = rhs_ref.shape
    alive = lax.broadcasted_iota(jnp.int32, (Y, S), 1) < counts_ref[lax.axis_index("gz")]
    inverse = jnp.sqrt(total_ref[0:1, S - 1 : S] / total_ref[0:1, 0:1])
    power = [jnp.ones_like(inverse)]
    for _ in range(DEGREE):
        power.append(power[-1] * inverse)
    answer, residue = chebyshev_polynomials()
    scale_sol = [jnp.broadcast_to(answer[i] * power[i + 1], (Y, S)) for i in range(DEGREE)]
    scale_res = [jnp.broadcast_to(residue[i] * power[i], (Y, S)) for i in range(DEGREE + 1)]
    for x in range(X):
        terms = [jnp.where(alive, rhs_ref[x], 0.0)] + [kry_ref[i, x] for i in range(DEGREE)]
        sol_ref[x] = sum(terms[i] * scale_sol[i] for i in range(DEGREE))
        res_ref[x] = sum(terms[i] * scale_res[i] for i in range(DEGREE + 1))


def on_device(sizes, right_side, coefficient, start_vector, plane_counts):
    X, Y, S = right_side.shape
    f32 = jnp.float32
    stages, floods = plan(sizes)
    most = max(len(offsets(sizes, axes)) for axes in stages)
    vmem = pl.BlockSpec(memory_space=pltpu.VMEM)
    krylov, total = pl.pallas_call(
        functools.partial(kernel, sizes),
        out_shape=(jax.ShapeDtypeStruct((DEGREE, X, Y, S), f32), jax.ShapeDtypeStruct((8, S), f32)),
        in_specs=[pl.BlockSpec(memory_space=pltpu.SMEM)] + [pl.BlockSpec(memory_space=pl.ANY)] * 3,
        out_specs=(pl.BlockSpec(memory_space=pl.ANY), vmem),
        scratch_shapes=[
            *[pltpu.VMEM((X, Y, S), f32)] * 3,
            pltpu.VMEM((POWER - 1, X, Y, S), f32),
            pltpu.VMEM((DEGREE, X, Y, S), f32),
            pltpu.VMEM((X + 1, Y, S), f32),
            *[pltpu.VMEM((X, Y, S), f32)] * 5,
            *[pltpu.VMEM((2, 8, Y, S), f32), pltpu.VMEM((2, 8, X, S), f32), pltpu.VMEM((2, 7, Y, S), f32)] * 2,
            pltpu.VMEM((len(stages), 8, S), f32),
            pltpu.VMEM((len(stages), -(-most // 8) * 8, S), f32),
            pltpu.SemaphoreType.DMA((3, 2)),
            pltpu.SemaphoreType.DMA((4, 3, 2)),
            pltpu.SemaphoreType.DMA((len(stages),)),
            pltpu.SemaphoreType.DMA((len(stages),)),
            pltpu.SemaphoreType.DMA((DEGREE,)),
            pltpu.SemaphoreType.REGULAR((max(floods, 1),)),
            pltpu.SemaphoreType.DMA((3,)),
        ],
        compiler_params=pltpu.CompilerParams(collective_id=0, has_side_effects=True),
    )(plane_counts, right_side, coefficient, start_vector)
    return pl.pallas_call(
        combine,
        out_shape=(jax.ShapeDtypeStruct((X, Y, S), f32),) * 2,
        in_specs=[pl.BlockSpec(memory_space=pltpu.SMEM), vmem, vmem, vmem],
        out_specs=(vmem, vmem),
    )(plane_counts, total, right_side, krylov)


def solution(mesh):
    sizes = {a: mesh.shape[a] for a in AXES}
    spec = P("gx", "gy", "gz")
    return jax.shard_map(
        functools.partial(on_device, sizes),
        mesh=mesh,
        in_specs=(spec, spec, spec, P()),
        out_specs=(spec, spec),
        check_vma=False,
    )
```

```python
import functools

import numpy as np
import jax
import jax.numpy as jnp
from jax import lax
from jax.experimental import pallas as pl
from jax.experimental.pallas import tpu as pltpu
from jax.sharding import PartitionSpec as P

POWER = 3
DEGREE = 4
AXES = ("gx", "gy", "gz")
DIRECT_LIMIT = 64
START, RIGHT, V1, V2, K1, K2, K3 = range(7)
ENTRIES = {START: (0, 2, 0), RIGHT: (2, 1, 2), V1: (3, 1, 1), V2: (4, 1, 0), K1: (5, 1, 3), K2: (6, 1, 2), K3: (7, 1, 3)}
MESH = pl.DeviceIdType.MESH


def chebyshev_polynomials():
    basis = np.zeros(DEGREE + 2)
    basis[0] = 1.0
    times = lambda poly: np.concatenate([[0.0], poly[:-1]])
    sharpness = 1.2
    ratio = 1.0 / sharpness
    answer = np.zeros_like(basis)
    residue = basis.copy()
    direction = basis / 0.6
    for section in range(DEGREE):
        answer = answer + direction
        residue = residue - times(direction)
        if section < DEGREE - 1:
            fresh = 1.0 / (2.0 * sharpness - ratio)
            direction = fresh * ratio * direction + 2.0 * fresh / 0.5 * residue
            ratio = fresh
    return [float(v) for v in answer[:DEGREE]], [float(v) for v in residue[: DEGREE + 1]]


def plan(sizes):
    if sizes["gx"] * sizes["gy"] * sizes["gz"] <= DIRECT_LIMIT:
        return (("gx", "gy", "gz"),), max(sum(sizes.values()) - len(sizes) - 2, 1)
    return (("gz",), ("gx",), ("gy",)), 0


def offsets(sizes, axes):
    grid = list(np.ndindex(*[sizes[a] for a in axes]))
    return [dict(zip(axes, map(int, o))) for o in grid if any(o)]


def kernel(
    sizes, counts_ref, rhs_hbm, coef_hbm, start_hbm, kry_out, total_ref, rhs_ref, coef_ref, start_ref,
    pow_ref, kry_ref, wx_ref, wym_ref, wyp_ref, wzm_ref, wzp_ref, diag_ref,
    sx, sy, sz, rx, ry, rz, own_ref, sums_ref, send_sem, recv_sem, sum_send, sum_recv, out_sem, flood_sem, in_sem,
):
    X, Y, S = rhs_ref.shape
    me = {a: lax.axis_index(a) for a in AXES}
    stages, floods = plan(sizes)
    loads = [
        pltpu.make_async_copy(src, dst, in_sem.at[i])
        for i, (src, dst) in enumerate(((coef_hbm, coef_ref), (start_hbm, start_ref), (rhs_hbm, rhs_ref)))
    ]
    for load in loads:
        load.start()
    has = {}
    for a in AXES:
        has[a] = (me[a] > 0, me[a] < sizes[a] - 1)
    neighbours = sum(h.astype(jnp.int32) for a in AXES for h in has[a])

    def greet(sem):
        for a in AXES:
            for side in (0, 1):
                @pl.when(has[a][side])
                def _(a=a, side=side):
                    pl.semaphore_signal(
                        sem, inc=1, device_id={a: me[a] + (1 if side else -1)}, device_id_type=MESH
                    )

    def flood(i):
        if i < floods:
            greet(flood_sem.at[i])

    def flood_wait(i):
        if i < floods:
            pl.semaphore_wait(flood_sem.at[i], neighbours)

    barrier = pltpu.get_barrier_semaphore()
    if floods:
        greet(barrier)
        arrivals = neighbours
    else:
        for a in AXES:
            for step in range(1, sizes[a]):
                pl.semaphore_signal(
                    barrier, inc=1, device_id={a: lax.rem(me[a] + step, sizes[a])}, device_id_type=MESH
                )
        arrivals = sum(sizes[a] - 1 for a in AXES)

    lane = lax.broadcasted_iota(jnp.int32, (Y, S), 1)
    row = lax.broadcasted_iota(jnp.int32, (Y, S), 0)
    planes = counts_ref[me["gz"]]
    alive = lane < planes
    is_first = lane == 0
    is_last = lane == planes - 1
    top = row == 0
    bottom = row == Y - 1

    def descriptor(msg, axis, side):
        send, recv, which = {"gx": (sx, rx, 0), "gy": (sy, ry, 1), "gz": (sz, rz, 2)}[axis]
        entry, fields, arrival = ENTRIES[msg]
        at = msg if axis == "gz" else pl.ds(entry, fields)
        return pltpu.make_async_remote_copy(
            src_ref=send.at[side, at],
            dst_ref=recv.at[1 - side, at],
            send_sem=send_sem.at[which, side],
            recv_sem=recv_sem.at[arrival, which, 1 - side],
            device_id={axis: me[axis] + (1 if side else -1)},
            device_id_type=MESH,
        )

    class Packer:
        def __init__(self, msg):
            self.msg = msg
            self.low = jnp.zeros((Y, S), jnp.float32)
            self.high = jnp.zeros((Y, S), jnp.float32)

        def put(self, f, x, value):
            e = ENTRIES[self.msg][0] + f
            if x == 0:
                sx[0, e] = value
            if x == X - 1:
                sx[1, e] = value
            sy[0, e, x : x + 1, :] = value[0:1, :]
            sy[1, e, x : x + 1, :] = value[Y - 1 : Y, :]
            here = lane == f * X + x
            self.low = jnp.where(here, value[:, 0:1], self.low)
            tail = jnp.sum(jnp.where(is_last, value, 0.0), axis=1, keepdims=True)
            self.high = jnp.where(here, tail, self.high)

        def finish(self):
            sz[0, self.msg] = self.low
            sz[1, self.msg] = self.high

    def launch(msg):
        for axis in AXES:
            for side in (0, 1):
                @pl.when(has[axis][side])
                def _(axis=axis, side=side):
                    descriptor(msg, axis, side).start()

    def receive(msg):
        for axis in AXES:
            for side in (0, 1):
                @pl.when(has[axis][1 - side])
                def _(axis=axis, side=side):
                    descriptor(msg, axis, side).wait_recv()

    def drain():
        for which, (axis, send, recv) in enumerate((("gx", sx, rx), ("gy", sy, ry), ("gz", sz, rz))):
            for side in (0, 1):
                @pl.when(has[axis][side])
                def _(axis=axis, side=side, which=which, send=send, recv=recv):
                    pltpu.make_async_remote_copy(
                        src_ref=send.at[side],
                        dst_ref=recv.at[1 - side],
                        send_sem=send_sem.at[which, side],
                        recv_sem=recv_sem.at[0, which, 1 - side],
                        device_id={axis: me[axis] + (1 if side else -1)},
                        device_id_type=MESH,
                    ).wait_send()

    def blank():
        for axis, recv in (("gx", rx), ("gy", ry), ("gz", rz)):
            for side in (0, 1):
                @pl.when(jnp.logical_not(has[axis][side]))
                def _(recv=recv, side=side):
                    recv[side] = jnp.zeros(recv.shape[1:], jnp.float32)

    def around(load, msg, f, x, zlow, zhigh):
        centre = load(x)
        below = rx[0, ENTRIES[msg][0] + f] if x == 0 else load(x - 1)
        above = rx[1, ENTRIES[msg][0] + f] if x == X - 1 else load(x + 1)
        ym = jnp.where(top, ry[0, ENTRIES[msg][0] + f, x : x + 1, :], pltpu.roll(centre, 1, 0))
        yp = jnp.where(bottom, ry[1, ENTRIES[msg][0] + f, x : x + 1, :], pltpu.roll(centre, Y - 1, 0))
        at = f * X + x
        zm = jnp.where(is_first, zlow[:, at : at + 1], pltpu.roll(centre, 1, 1))
        zp = jnp.where(is_last, zhigh[:, at : at + 1], pltpu.roll(centre, S - 1, 1))
        return centre, below, above, ym, yp, zm, zp

    def face(centre, other):
        other = jnp.where(other > 0, other, centre)
        return jnp.where(alive, 0.5 * (centre + other), 0.0)

    def weights(msg):
        zlow, zhigh = rz[0, msg], rz[1, msg]
        under = None
        for x in range(X):
            c, below, above, ym, yp, zm, zp = around(lambda i: coef_ref[i], msg, 0, x, zlow, zhigh)
            if x == 0:
                under = face(c, below)
                wx_ref[0] = under
            over = face(c, above)
            parts = [face(c, o) for o in (ym, yp, zm, zp)]
            wx_ref[x + 1] = over
            wym_ref[x], wyp_ref[x], wzm_ref[x], wzp_ref[x] = parts
            diag_ref[x] = (under + over) + (parts[0] + parts[1]) + (parts[2] + parts[3])
            under = over

    def operate(load, msg, f, emit):
        zlow, zhigh = rz[0, msg], rz[1, msg]
        for x in range(X):
            c, below, above, ym, yp, zm, zp = around(load, msg, f, x, zlow, zhigh)
            near = wx_ref[x] * below + wx_ref[x + 1] * above
            near = near + (wym_ref[x] * ym + wyp_ref[x] * yp)
            near = near + (wzm_ref[x] * zm + wzp_ref[x] * zp)
            emit(x, diag_ref[x] * c - near)

    def step(load, msg, f, store, out_msg, total=None):
        pack = Packer(out_msg) if out_msg is not None else None
        box = [total]

        def emit(x, value):
            if store is not None:
                store[x] = value
            if pack is not None:
                pack.put(0, x, value)
            if total is not None:
                box[0] = box[0] + value * value

        operate(load, msg, f, emit)
        if pack is not None:
            pack.finish()
            launch(out_msg)
        return box[0]

    blank()
    loads[0].wait()
    loads[1].wait()
    pack = Packer(START)
    for x in range(X):
        pack.put(0, x, coef_ref[x])
        pack.put(1, x, start_ref[x])
    pack.finish()
    pl.semaphore_wait(barrier, arrivals)
    flood(0)
    launch(START)
    loads[2].wait()
    pack = Packer(RIGHT)
    for x in range(X):
        pack.put(0, x, rhs_ref[x])
    pack.finish()
    launch(RIGHT)

    def out_copy(i):
        return pltpu.make_async_copy(kry_ref.at[i], kry_out.at[i], out_sem.at[i])

    def krylov(i):
        source, msg, out_msg = ((None, RIGHT, K1), (0, K1, K2), (1, K2, K3), (2, K3, None))[i]
        load = (lambda x: rhs_ref[x]) if source is None else (lambda x: kry_ref[source, x])
        receive(msg)
        step(load, msg, 0, kry_ref.at[i], out_msg)
        out_copy(i).start()

    zero = jnp.zeros((Y, S), jnp.float32)
    flood_wait(0)
    for i in range(1, floods - 2):
        flood(i)
        flood_wait(i)
    receive(START)
    weights(START)
    step(lambda x: start_ref[x], START, 1, pow_ref.at[0], V1)
    krylov(0)
    receive(V1)
    if floods > 2:
        flood(floods - 2)
    lower = step(lambda x: pow_ref[0, x], V1, 0, pow_ref.at[1], V2, zero)
    if floods > 2:
        flood_wait(floods - 2)
    if floods > 1:
        flood(floods - 1)
    krylov(1)
    if floods > 1:
        flood_wait(floods - 1)
    receive(V2)
    upper = step(lambda x: pow_ref[1, x], V2, 0, None, None, zero)

    pick = lax.broadcasted_iota(jnp.int32, (8, S), 1) < S // 2
    total = jnp.where(pick, jnp.sum(upper, keepdims=True), jnp.sum(lower, keepdims=True))

    def sum_copy(k, slot, offset):
        return pltpu.make_async_remote_copy(
            src_ref=own_ref.at[k, pl.ds(0, 1)],
            dst_ref=sums_ref.at[k, pl.ds(slot, 1)],
            send_sem=sum_send.at[k],
            recv_sem=sum_recv.at[k],
            device_id={a: lax.rem(me[a] + d, sizes[a]) for a, d in offset.items()},
            device_id_type=MESH,
        )

    def all_sums(k, count):
        whole = sums_ref.at[k, pl.ds(0, count)]
        return pltpu.make_async_remote_copy(
            src_ref=whole,
            dst_ref=whole,
            send_sem=sum_send.at[k],
            recv_sem=sum_recv.at[k],
            device_id={"gz": lax.rem(me["gz"] + 1, sizes["gz"])},
            device_id_type=MESH,
        )

    for k, axes in enumerate(stages):
        own_ref[k] = total
        others = offsets(sizes, axes)
        for slot, offset in enumerate(others):
            sum_copy(k, slot, offset).start()
        if k == 0:
            krylov(2)
        if k == len(stages) - 1:
            krylov(3)
        all_sums(k, len(others)).wait_recv()
        total = total + jnp.sum(sums_ref[k, 0 : len(others), :], axis=0, keepdims=True)
    total_ref[...] = total
    for i in range(DEGREE):
        out_copy(i).wait()
    drain()
    for k, axes in enumerate(stages):
        all_sums(k, len(offsets(sizes, axes))).wait_send()


def combine(counts_ref, total_ref, rhs_ref, kry_ref, sol_ref, res_ref):
    X, Y, S = rhs_ref.shape
    alive = lax.broadcasted_iota(jnp.int32, (Y, S), 1) < counts_ref[lax.axis_index("gz")]
    inverse = jnp.sqrt(total_ref[0:1, S - 1 : S] / total_ref[0:1, 0:1])
    power = [jnp.ones_like(inverse)]
    for _ in range(DEGREE):
        power.append(power[-1] * inverse)
    answer, residue = chebyshev_polynomials()
    scale_sol = [jnp.broadcast_to(answer[i] * power[i + 1], (Y, S)) for i in range(DEGREE)]
    scale_res = [jnp.broadcast_to(residue[i] * power[i], (Y, S)) for i in range(DEGREE + 1)]
    for x in range(X):
        terms = [jnp.where(alive, rhs_ref[x], 0.0)] + [kry_ref[i, x] for i in range(DEGREE)]
        sol_ref[x] = sum(terms[i] * scale_sol[i] for i in range(DEGREE))
        res_ref[x] = sum(terms[i] * scale_res[i] for i in range(DEGREE + 1))


def on_device(sizes, right_side, coefficient, start_vector, plane_counts):
    X, Y, S = right_side.shape
    f32 = jnp.float32
    stages, floods = plan(sizes)
    most = max(len(offsets(sizes, axes)) for axes in stages)
    vmem = pl.BlockSpec(memory_space=pltpu.VMEM)
    krylov, total = pl.pallas_call(
        functools.partial(kernel, sizes),
        out_shape=(jax.ShapeDtypeStruct((DEGREE, X, Y, S), f32), jax.ShapeDtypeStruct((8, S), f32)),
        in_specs=[pl.BlockSpec(memory_space=pltpu.SMEM)] + [pl.BlockSpec(memory_space=pl.ANY)] * 3,
        out_specs=(pl.BlockSpec(memory_space=pl.ANY), vmem),
        scratch_shapes=[
            *[pltpu.VMEM((X, Y, S), f32)] * 3,
            pltpu.VMEM((POWER - 1, X, Y, S), f32),
            pltpu.VMEM((DEGREE, X, Y, S), f32),
            pltpu.VMEM((X + 1, Y, S), f32),
            *[pltpu.VMEM((X, Y, S), f32)] * 5,
            *[pltpu.VMEM((2, 8, Y, S), f32), pltpu.VMEM((2, 8, X, S), f32), pltpu.VMEM((2, 7, Y, S), f32)] * 2,
            pltpu.VMEM((len(stages), 8, S), f32),
            pltpu.VMEM((len(stages), -(-most // 8) * 8, S), f32),
            pltpu.SemaphoreType.DMA((3, 2)),
            pltpu.SemaphoreType.DMA((4, 3, 2)),
            pltpu.SemaphoreType.DMA((len(stages),)),
            pltpu.SemaphoreType.DMA((len(stages),)),
            pltpu.SemaphoreType.DMA((DEGREE,)),
            pltpu.SemaphoreType.REGULAR((max(floods, 1),)),
            pltpu.SemaphoreType.DMA((3,)),
        ],
        compiler_params=pltpu.CompilerParams(collective_id=0, has_side_effects=True),
    )(plane_counts, right_side, coefficient, start_vector)
    return pl.pallas_call(
        combine,
        out_shape=(jax.ShapeDtypeStruct((X, Y, S), f32),) * 2,
        in_specs=[pl.BlockSpec(memory_space=pltpu.SMEM), vmem, vmem, vmem],
        out_specs=(vmem, vmem),
    )(plane_counts, total, right_side, krylov)


def solution(mesh):
    sizes = {a: mesh.shape[a] for a in AXES}
    spec = P("gx", "gy", "gz")
    return jax.shard_map(
        functools.partial(on_device, sizes),
        mesh=mesh,
        in_specs=(spec, spec, spec, P()),
        out_specs=(spec, spec),
        check_vma=False,
    )
```
